32 devices in a mesh: dp: 4 (over y, x), expert: 8 (over z, core).
Axes of the slice: x: 2, y: 2, z: 4, core: 2. Of those that a mesh axis runs over, the one named last changes fastest.
Arguments:
- tokens: bfloat16 [8, 512, 4096], P('expert', 'dp'), may hold values from -6 to 6
- w_gate: bfloat16 [8, 4096, 896], P('expert'), may hold values from -0.09375 to 0.09375
- w_up: bfloat16 [8, 4096, 896], P('expert'), may hold values from -0.09375 to 0.09375
- w_down: bfloat16 [8, 896, 4096], P('expert'), may hold values from -0.1875 to 0.1875
- expert_ids: int32 [8, 512, 4], P('expert'), may hold values from 0 to 7, all different within a row
- gate_index: int32 [8, 512, 4], P('expert'), may hold values from 0 to 255
- gate_table: float32 [256], replicated, may hold values from 0.05 to 1
- spill: int32 [8, 512], P('expert'), may hold values from 0 to 3, as said below
Outputs:
- mixed: bfloat16 [8, 512, 4096], P('expert', 'dp')
The draws below stay inside these ranges and needn't reach their ends.
Inputs may be any that keep to these rules, and one draw needn't show every extreme that they name: `spill`: A token is dispatched by a device of its own column. Of the 128 tokens of one device at most 32 are dispatched by any one other device, and in every draw some device hands exactly 32 to some peer.
All inputs are finite; a program needn't handle non-finite values.
Results may differ from the reference program's by a relative error of at most 0.0058.
Values may be sent and summed in bfloat16 or wider, within the bound.
A program may use at most 128 MiB of HBM per device.

```python
import math
import jax
import jax.numpy as jnp
from jax import lax

D = 4096
FF = 896
TOP = 4
LEVELS = 256
TOK_DEV = 128
EXPERTS = 8
NCOL = 8
COL_TOK = 512
CAP = 96
SPILL = 32
N_DP = 4


def draw_spill(key, part):

    def column(column_key):
        count_key, perm_key, pick_key = jax.random.split(column_key, 3)
        counts = jax.random.randint(count_key, (N_DP, N_DP - 1), 0, SPILL + 1)
        full_home = jax.random.randint(pick_key, (), 0, N_DP)
        counts = counts.at[full_home, 0].set(SPILL)
        bounds = jnp.cumsum(counts, axis=1)
        positions = jax.vmap(lambda home_key: jax.random.permutation(home_key, TOK_DEV))(jax.random.split(perm_key, N_DP))
        passed = jnp.sum((positions[:, :, None] >= bounds[:, None, :]).astype(jnp.int32), axis=2)
        home_dev = jnp.arange(N_DP, dtype=jnp.int32)[:, None]
        senders = jnp.where(passed < N_DP - 1, (home_dev + 1 + passed) % N_DP, home_dev)
        return senders.reshape(-1).astype(jnp.int32)
    column_keys = jax.random.split(jax.random.fold_in(key, 17), NCOL)
    return jax.vmap(column)(column_keys)


def with_ends(result, stream_key, least, top_value):
    spot = [jax.random.randint(jax.random.fold_in(stream_key, axis), (), 0, length) for axis, length in enumerate(result.shape)]
    longest = result.shape.index(max(result.shape))
    next_to = spot[:longest] + [(spot[longest] + 1) % result.shape[longest]] + spot[longest + 1:]
    return result.at[tuple(spot)].set(least).at[tuple(next_to)].set(top_value)


def steps_of(stream_key, dims, pieces, low, largest):
    level = 1.0
    for position, parts in pieces:
        steps = jax.random.uniform(jax.random.fold_in(jax.random.fold_in(stream_key, 6), position), (parts,), jnp.float32, low / len(pieces), largest / len(pieces))
        level = level * jnp.repeat(jnp.exp(steps), dims[position] // parts).reshape((-1,) + (1,) * (len(dims) - 1 - position))
    return level


def different_ones(own_key, rows, number_of, top, lift):
    order = jax.random.permutation(jax.random.fold_in(own_key, 1), number_of)
    pull = order
    for power in range(3):
        pull = pull * pull // number_of
    pull = pull * lift // number_of
    chance = jax.random.randint(jax.random.fold_in(own_key, 2), (rows, number_of), 0, 4096) + pull
    fixed_rows = jax.random.permutation(jax.random.fold_in(own_key, 3), rows)[jnp.arange(number_of) % rows]
    chance = jnp.where(jnp.arange(rows)[:, None] == fixed_rows[None, :], 1 << 14, chance)
    priority = chance * number_of + jnp.arange(number_of)
    return lax.top_k(priority.astype(jnp.int32), top)[1].astype(jnp.int32)


def bell_draw(stream_key, shape, spread, bound, cuts=(), kind=jnp.bfloat16):
    values = jax.random.normal(stream_key, shape, jnp.float32) * spread
    if len(cuts) > 0:
        values = steps_of(stream_key, shape, cuts, -0.22, 0.18) * values
    return jnp.clip(values, min=-bound, max=bound).astype(kind)


def setup_inputs(seed: int = 0) -> dict:
    seeds = jax.random.split(jax.random.key(seed), 9)
    tokens = bell_draw(seeds[0], (NCOL, COL_TOK, D), 1.0, 6.0, ((0, 8), (1, 4)))
    w_gate = bell_draw(seeds[1], (EXPERTS, D, FF), D ** -0.5, 0.09375, ((0, 8),))
    w_up = bell_draw(seeds[2], (EXPERTS, D, FF), D ** -0.5, 0.09375, ((0, 8),))
    w_down = bell_draw(seeds[3], (EXPERTS, FF, D), FF ** -0.5, 0.1875, ((0, 8),))
    expert_ids = different_ones(seeds[4], NCOL * COL_TOK, EXPERTS, TOP, 8192).reshape((NCOL, COL_TOK, TOP))
    gate_index = with_ends(jax.random.randint(seeds[5], (NCOL, COL_TOK, TOP), 0, LEVELS), jax.random.fold_in(seeds[5], 1), 0, LEVELS - 1).astype(jnp.int32)
    gate_table = jnp.clip(jnp.exp(jax.random.uniform(seeds[6], (LEVELS,), jnp.float32, math.log(0.05), math.log(1.0))), 0.05, 1.0)
    spill = draw_spill(jax.random.fold_in(seeds[8], 71), 0)
    return dict(tokens=tokens, w_gate=w_gate, w_up=w_up, w_down=w_down, expert_ids=expert_ids, gate_index=gate_index, gate_table=gate_table, spill=spill)


def rank_within(route_row, key_count):
    onehot = (route_row[:, None] == jnp.arange(key_count, dtype=jnp.int32)[None, :]).astype(jnp.int32)
    return jnp.sum((jnp.cumsum(onehot, axis=0) - onehot) * onehot, axis=1).astype(jnp.int32)


def reference(tokens, w_gate, w_up, w_down, expert_ids, gate_index, gate_table, spill):
    ncol_count = tokens.shape[0]
    column_tokens = tokens.shape[1]
    model_width = tokens.shape[2]
    experts_all = w_gate.shape[0]
    top_count = expert_ids.shape[2]
    picked = gate_table[gate_index]
    weight = picked / jnp.sum(picked, axis=-1, keepdims=True)
    pair_sender = jnp.repeat(spill, top_count, axis=1).astype(jnp.int32)
    flat_ids = expert_ids.reshape(ncol_count, column_tokens * top_count).astype(jnp.int32)
    route_key = pair_sender * experts_all + flat_ids
    slot_rank = lax.map(lambda row: rank_within(row, N_DP * experts_all), route_key)
    is_kept = slot_rank < CAP
    per_expert = ncol_count * N_DP * CAP
    column_base = jnp.arange(ncol_count, dtype=jnp.int32)[:, None]
    slot_index = (column_base * N_DP + pair_sender) * CAP + slot_rank
    slot_index = jnp.where(is_kept, slot_index, per_expert).astype(jnp.int32)
    token_total = ncol_count * column_tokens
    pair_token = column_base * column_tokens + jnp.arange(column_tokens * top_count, dtype=jnp.int32)[None, :] // top_count
    row_source = jnp.full((experts_all, per_expert + 1), token_total, jnp.int32)
    row_source = row_source.at[flat_ids, slot_index].set(pair_token.astype(jnp.int32))[:, :per_expert]
    kept_weight = jnp.where(is_kept, weight.reshape(ncol_count, column_tokens * top_count), 0.0).astype(jnp.float32)
    row_scale = jnp.zeros((experts_all, per_expert + 1), jnp.float32)
    row_scale = row_scale.at[flat_ids, slot_index].set(kept_weight)[:, :per_expert]
    padded = jnp.concatenate([tokens.reshape(token_total, model_width), jnp.zeros((1, model_width), tokens.dtype)], axis=0)

    def expert_step(totals, inputs):
        gate_mat, up_mat, down_mat, sources, scales = inputs
        rows_in = padded[sources]
        gate_part = jnp.dot(rows_in, gate_mat, preferred_element_type=jnp.float32)
        up_part = jnp.dot(rows_in, up_mat, preferred_element_type=jnp.float32)
        hidden = (jax.nn.silu(gate_part) * up_part).astype(jnp.bfloat16)
        expert_out = jnp.dot(hidden, down_mat, preferred_element_type=jnp.float32).astype(jnp.bfloat16)
        totals = totals.at[sources].add(scales[:, None] * expert_out.astype(jnp.float32))
        return totals, None

    start = jnp.zeros((token_total + 1, model_width), jnp.float32)
    totals, unused = lax.scan(expert_step, start, (w_gate, w_up, w_down, row_source, row_scale))
    return totals[:token_total].astype(jnp.bfloat16).reshape(ncol_count, column_tokens, model_width)
```

```python
import functools
import jax
import jax.numpy as jnp
from jax import lax
from jax.experimental import pallas as pl
from jax.experimental.pallas import tpu as pltpu
from jax.sharding import PartitionSpec as P


def exchange_plan(tokens, w_gate, w_up, w_down, expert_ids, gate_index, gate_table, spill):
    dp_count = lax.axis_size("dp")
    expert_count = lax.axis_size("expert")
    local_experts = w_gate.shape[0]
    experts_all = local_experts * expert_count
    own_rows = tokens.shape[1]
    model_width = tokens.shape[2]
    column_tokens = spill.shape[1]
    top_count = expert_ids.shape[2]
    capacity = 3 * own_rows * top_count // (2 * experts_all)
    spill_room = own_rows // 4
    dp_index = lax.axis_index("dp")
    senders = spill[0]
    flat_ids = expert_ids[0].reshape(-1)
    level_count = gate_table.shape[0]
    matches = gate_index[0][:, :, None] == jnp.arange(level_count, dtype=jnp.int32)
    picked = jnp.sum(jnp.where(matches, gate_table, 0.0), axis=2)
    weight = picked / jnp.sum(picked, axis=1, keepdims=True)
    pair_sender = jnp.repeat(senders, top_count)
    is_mine = pair_sender == dp_index
    onehot = (
        (flat_ids[:, None] == jnp.arange(experts_all, dtype=jnp.int32)) & is_mine[:, None]
    ).astype(jnp.int32)
    slot_rank = jnp.sum((jnp.cumsum(onehot, axis=0) - onehot) * onehot, axis=1)
    is_kept = is_mine & (slot_rank < capacity)
    empty_slot = experts_all * capacity
    slot_index = jnp.where(is_kept, flat_ids * capacity + slot_rank, empty_slot)
    pair_token = jnp.arange(column_tokens * top_count, dtype=jnp.int32) // top_count
    zero_row = jnp.zeros((1, model_width), tokens.dtype)
    token_ids = jnp.arange(column_tokens, dtype=jnp.int32)
    home_dev = token_ids // own_rows
    local_token = token_ids - home_dev * own_rows
    is_moved = senders != home_dev
    route_key = home_dev * dp_count + senders
    route_hot = (route_key[:, None] == jnp.arange(dp_count * dp_count, dtype=jnp.int32)).astype(
        jnp.int32
    )
    spill_rank = jnp.sum((jnp.cumsum(route_hot, axis=0) - route_hot) * route_hot, axis=1)
    incoming = is_moved & (senders == dp_index)
    spill_slots = dp_count * spill_room
    outgoing = is_moved & (home_dev == dp_index)
    send_target = jnp.where(outgoing, senders * spill_room + spill_rank, spill_slots)
    send_source = (
        jnp.full((spill_slots,), own_rows, jnp.int32).at[send_target].set(local_token, mode="drop")
    )
    own_padded = jnp.concatenate([tokens[0], zero_row], axis=0)
    outgoing_rows = own_padded[send_source].reshape(dp_count, spill_room, model_width)
    arrived = lax.all_to_all(outgoing_rows, "dp", split_axis=0, concat_axis=0, tiled=True)
    source_rows = jnp.concatenate(
        [tokens[0], arrived.reshape(spill_slots, model_width), zero_row], axis=0
    )
    token_row = jnp.where(
        home_dev == dp_index,
        local_token,
        jnp.where(incoming, own_rows + home_dev * spill_room + spill_rank, own_rows + spill_slots),
    )
    dispatch_source = (
        jnp.full((empty_slot,), source_rows.shape[0] - 1, jnp.int32)
        .at[slot_index]
        .set(token_row[pair_token], mode="drop")
    )
    outbound = source_rows[dispatch_source].reshape(
        expert_count, local_experts, capacity, model_width
    )
    block = lax.all_to_all(outbound, "expert", split_axis=0, concat_axis=0, tiled=True)
    gate_part = jnp.einsum("aecd,edf->aecf", block, w_gate, preferred_element_type=jnp.float32)
    up_part = jnp.einsum("aecd,edf->aecf", block, w_up, preferred_element_type=jnp.float32)
    hidden = (jax.nn.silu(gate_part) * up_part).astype(jnp.bfloat16)
    expert_out = jnp.einsum(
        "aecf,efd->aecd", hidden, w_down, preferred_element_type=jnp.float32
    ).astype(jnp.bfloat16)
    returned = lax.all_to_all(expert_out, "expert", split_axis=0, concat_axis=0, tiled=True)
    results = jnp.concatenate([returned.reshape(empty_slot, model_width), zero_row], axis=0)
    slot_grid = jnp.concatenate(
        [
            slot_index.reshape(column_tokens, top_count),
            jnp.full((1, top_count), empty_slot, jnp.int32),
        ],
        axis=0,
    )
    kept_scale = jnp.where(is_kept.reshape(column_tokens, top_count), weight, 0.0)
    scale_grid = jnp.concatenate([kept_scale, jnp.zeros((1, top_count), jnp.float32)], axis=0)

    def combine(chosen):
        chosen_slots = slot_grid[chosen]
        chosen_scale = scale_grid[chosen]
        summed = jnp.zeros((chosen.shape[0], model_width), jnp.float32)
        for member in range(top_count):
            summed = summed + chosen_scale[:, member : member + 1] * results[
                chosen_slots[:, member]
            ].astype(jnp.float32)
        return summed

    own_ids = dp_index * own_rows + jnp.arange(own_rows, dtype=jnp.int32)
    own_part = combine(own_ids)
    arrived_target = jnp.where(incoming, home_dev * spill_room + spill_rank, spill_slots)
    arrived_ids = (
        jnp.full((spill_slots,), column_tokens, jnp.int32)
        .at[arrived_target]
        .set(token_ids, mode="drop")
    )
    arrived_part = combine(arrived_ids).reshape(dp_count, spill_room, model_width)
    returned_part = lax.all_to_all(
        arrived_part.astype(jnp.bfloat16), "dp", split_axis=0, concat_axis=0, tiled=True
    ).astype(arrived_part.dtype)
    back_rows = jnp.concatenate(
        [returned_part.reshape(spill_slots, model_width), jnp.zeros((1, model_width), jnp.float32)],
        axis=0,
    )
    back_pick = jnp.where(
        is_moved[own_ids], senders[own_ids] * spill_room + spill_rank[own_ids], spill_slots
    )
    mixed = own_part + back_rows[back_pick]
    return mixed.astype(jnp.bfloat16)[None]


CORES = 2
CHUNKS = 8
LAG = 2
MESH = pl.DeviceIdType.MESH


def token_scales(expert_ids, gate_index, gate_table, spill, own_rows, experts_all):
    top_count = expert_ids.shape[2]
    column_tokens = spill.shape[1]
    capacity = 3 * own_rows * top_count // (2 * experts_all)
    first = lax.axis_index("dp") * own_rows
    senders = spill[0]
    experts = jnp.arange(experts_all, dtype=jnp.int32)
    hot = expert_ids[0][:, :, None] == experts
    chosen = jnp.any(hot, axis=1)
    own_senders = lax.dynamic_slice_in_dim(senders, first, own_rows)
    own_tokens = first + jnp.arange(own_rows, dtype=jnp.int32)
    earlier = (jnp.arange(column_tokens, dtype=jnp.int32)[None, :] < own_tokens[:, None]) & (
        senders[None, :] == own_senders[:, None]
    )
    rank = jnp.dot(
        earlier.astype(jnp.bfloat16), chosen.astype(jnp.bfloat16), preferred_element_type=jnp.float32
    )
    own_index = lax.dynamic_slice_in_dim(gate_index[0], first, own_rows)
    levels = jnp.arange(gate_table.shape[0], dtype=jnp.int32)
    picked = jnp.sum(jnp.where(own_index[:, :, None] == levels, gate_table, 0.0), axis=2)
    weight = picked / jnp.sum(picked, axis=1, keepdims=True)
    own_hot = lax.dynamic_slice_in_dim(hot, first, own_rows)
    scale = jnp.sum(jnp.where(own_hot, weight[:, :, None], 0.0), axis=1)
    return jnp.where(rank < capacity, scale, 0.0).T


def line_kernel(
    chips, tok, w_gate, w_up, w_down, scale, out,
    x, w_in, w_out, scales, both, hid, part, near, from_left, from_right, going, total,
    own_sem, sc_s, sc_r, ag_right, ag_left, ag_r, ag_sib, sib_r, part_s, part_r, go_s, left_r, right_r,
):
    own_rows, width = tok.shape[1], tok.shape[2]
    hidden_units = w_gate.shape[2]
    piece = own_rows // CHUNKS
    count = chips * CORES
    me = lax.axis_index("expert")
    p = me // CORES
    q = lax.rem(me, CORES)
    sib = p * CORES + 1 - q
    right, left = me + CORES, me - CORES
    has_right, has_left = p < chips - 1, p > 0

    def send(src, dst, send_sem, recv_sem, device):
        return pltpu.make_async_remote_copy(
            src_ref=src, dst_ref=dst, send_sem=send_sem, recv_sem=recv_sem,
            device_id={"expert": device}, device_id_type=MESH,
        )

    def rows(c):
        return pl.ds(pl.multiple_of(c * piece, piece), piece)

    def gather_copy(s, c, sems, recv, device):
        block = x.at[CORES * s + q, rows(c)]
        return send(block, block, sems.at[s, c], recv.at[s, c], device)

    loads = [
        pltpu.make_async_copy(tok.at[0], x.at[me], own_sem.at[0]),
        pltpu.make_async_copy(scale, scales.at[me], own_sem.at[1]),
        pltpu.make_async_copy(w_gate.at[0], w_in.at[:, pl.ds(0, hidden_units)], own_sem.at[2]),
        pltpu.make_async_copy(w_up.at[0], w_in.at[:, pl.ds(hidden_units, hidden_units)], own_sem.at[3]),
        pltpu.make_async_copy(w_down.at[0], w_out, own_sem.at[4]),
    ]
    loads[0].start()
    loads[1].start()
    barrier = pltpu.get_barrier_semaphore()
    for step in range(1, count):
        pl.semaphore_signal(
            barrier, inc=1, device_id={"expert": lax.rem(me + step, count)}, device_id_type=MESH
        )
    pl.semaphore_wait(barrier, count - 1)
    loads[0].wait()

    def first_sends(c, carry):
        @pl.when(has_right)
        def _():
            gather_copy(p, c, ag_right, ag_r, right).start()

        @pl.when(has_left)
        def _():
            gather_copy(p, c, ag_left, ag_r, left).start()

        gather_copy(p, c, ag_sib, sib_r, sib).start()
        return carry

    lax.fori_loop(0, CHUNKS, first_sends, 0)
    loads[1].wait()
    for step in range(1, count):
        send(
            scale, scales.at[me], sc_s.at[step], sc_r.at[step], lax.rem(me + step, count)
        ).start()
    for load in loads[2:]:
        load.start()
    for load in loads[2:]:
        load.wait()
    for step in range(1, count):
        send(
            scale, scales.at[lax.rem(me - step + count, count)], sc_s.at[step], sc_r.at[step], sib
        ).wait_recv()

    tall = CORES * own_rows
    in_tile = 2 * hidden_units // 7 if (2 * hidden_units) % 7 == 0 else 2 * hidden_units
    out_tile = width // 8

    def sib_wait(s):
        def one(c, carry):
            block = x.at[CORES * s + 1 - q, rows(c)]
            send(block, block, ag_sib.at[s, c], sib_r.at[s, c], sib).wait_recv()
            return carry

        lax.fori_loop(0, CHUNKS, one, 0)

    def expert(s):
        def enter(t, carry):
            cols = pl.ds(pl.multiple_of(t * in_tile, 128), in_tile)
            tokens = x[pl.ds(CORES * s, CORES)].reshape(tall, width)
            both[:, cols] = jnp.dot(tokens, w_in[:, cols], preferred_element_type=jnp.float32)
            return carry

        lax.fori_loop(0, 2 * hidden_units // in_tile, enter, 0)
        for core in range(CORES):
            part_rows = pl.ds(core * own_rows, own_rows)
            row = scales[CORES * s + core, pl.ds(me, 1), :]
            col = jnp.transpose(jnp.broadcast_to(row, (own_rows, own_rows)))[:, :1]
            gate = both[part_rows, pl.ds(0, hidden_units)]
            up = both[part_rows, pl.ds(hidden_units, hidden_units)]
            hid[part_rows, :] = (gate / (1.0 + jnp.exp(-gate)) * up * col).astype(hid.dtype)

        def leave(t, carry):
            cols = pl.ds(pl.multiple_of(t * out_tile, 128), out_tile)
            made = jnp.dot(hid[...], w_out[:, cols], preferred_element_type=jnp.float32)
            part[pl.ds(CORES * s, CORES), :, cols] = made.astype(part.dtype).reshape(
                CORES, own_rows, out_tile
            )
            return carry

        lax.fori_loop(0, width // out_tile, leave, 0)
        near_copy(s).start()

    def near_copy(s):
        return send(part.at[CORES * s + 1 - q], near.at[s], part_s.at[s], part_r.at[s], sib)

    def pair_sum(s, c):
        return part[CORES * s + q, rows(c)].astype(jnp.float32) + near[s, rows(c)].astype(jnp.float32)

    def onward(s, c, has_up, came, came_sem, device):
        @pl.when(c == 0)
        def _():
            near_copy(s).wait_recv()

        total[...] = pair_sum(s, c)

        @pl.when(has_up)
        def _():
            send(
                going.at[s, rows(c)], came.at[s, rows(c)], go_s.at[s, c], came_sem.at[s, c], sib
            ).wait_recv()
            total[...] += came[s, rows(c)].astype(jnp.float32)

        going[s, rows(c)] = total[...].astype(going.dtype)
        send(
            going.at[s, rows(c)], came.at[s, rows(c)], go_s.at[s, c], came_sem.at[s, c], device
        ).start()

    def slot(k, carry):
        for side in range(2):
            s = p - k if side == 0 else p + k
            valid = (s >= 0) if side == 0 else ((s < chips) & (k > 0))

            @pl.when(valid)
            def _():
                sib_wait(s)
                expert(s)

        def step(i, inner):
            to_right = i - LAG * p

            @pl.when((p < k) & (to_right >= 0) & (to_right < CHUNKS))
            def _():
                onward(k, to_right, has_left, from_left, left_r, right)

            to_left = i - LAG * (chips - 1 - p)
            low = chips - 1 - k

            @pl.when((p > low) & (to_left >= 0) & (to_left < CHUNKS))
            def _():
                onward(low, to_left, has_right, from_right, right_r, left)

            before = p - k - 1

            @pl.when((i < CHUNKS) & (before >= 0))
            def _():
                gather_copy(before, i, ag_right, ag_r, sib).wait_recv()

                @pl.when(has_right)
                def _():
                    gather_copy(before, i, ag_right, ag_r, right).start()

                gather_copy(before, i, ag_sib, sib_r, sib).start()

            after = p + k + 1

            @pl.when((i < CHUNKS) & (after < chips))
            def _():
                gather_copy(after, i, ag_left, ag_r, sib).wait_recv()

                @pl.when(has_left)
                def _():
                    gather_copy(after, i, ag_left, ag_r, left).start()

                gather_copy(after, i, ag_sib, sib_r, sib).start()

            return inner

        lax.fori_loop(0, CHUNKS + LAG * (chips - 1), step, 0)
        return carry

    lax.fori_loop(0, chips, slot, 0)
    near_copy(p).wait_recv()

    def finish(c, carry):
        total[...] = pair_sum(p, c)

        @pl.when(has_left)
        def _():
            block = from_left.at[p, rows(c)]
            send(block, block, go_s.at[p, c], left_r.at[p, c], sib).wait_recv()
            total[...] += from_left[p, rows(c)].astype(jnp.float32)

        @pl.when(has_right)
        def _():
            block = from_right.at[p, rows(c)]
            send(block, block, go_s.at[p, c], right_r.at[p, c], sib).wait_recv()
            total[...] += from_right[p, rows(c)].astype(jnp.float32)

        out[0, rows(c)] = total[...].astype(out.dtype)
        return carry

    lax.fori_loop(0, CHUNKS, finish, 0)

    for step in range(1, count):
        send(scale, scales.at[me], sc_s.at[step], sc_r.at[step], sib).wait_send()

    def drain(s, carry):
        near_copy(s).wait_send()

        def one(c, inner):
            gather_copy(s, c, ag_sib, sib_r, sib).wait_send()

            @pl.when(has_right & (s <= p))
            def _():
                gather_copy(s, c, ag_right, ag_r, sib).wait_send()

            @pl.when(has_left & (s >= p))
            def _():
                gather_copy(s, c, ag_left, ag_r, sib).wait_send()

            @pl.when(s != p)
            def _():
                block = going.at[s, rows(c)]
                send(block, block, go_s.at[s, c], left_r.at[s, c], sib).wait_send()

            return inner

        lax.fori_loop(0, CHUNKS, one, 0)
        return carry

    lax.fori_loop(0, chips, drain, 0)


def scratch_of(chips, own_rows, width, hidden_units, experts_all, dtype):
    count = chips * CORES
    blocks = pltpu.VMEM((count, own_rows, width), dtype)
    halves = pltpu.VMEM((chips, own_rows, width), dtype)
    dma = pltpu.SemaphoreType.DMA
    grid = dma((chips, CHUNKS))
    return [
        blocks,
        pltpu.VMEM((width, 2 * hidden_units), dtype),
        pltpu.VMEM((hidden_units, width), dtype),
        pltpu.VMEM((count, experts_all, own_rows), jnp.float32),
        pltpu.VMEM((CORES * own_rows, 2 * hidden_units), jnp.float32),
        pltpu.VMEM((CORES * own_rows, hidden_units), dtype),
        blocks,
        halves,
        halves,
        halves,
        halves,
        pltpu.VMEM((own_rows // CHUNKS, width), jnp.float32),
        dma((5,)),
        dma((count,)),
        dma((count,)),
        grid, grid, grid, grid, grid,
        dma((chips,)),
        dma((chips,)),
        grid, grid, grid,
    ]


def line_plan(tokens, w_gate, w_up, w_down, expert_ids, gate_index, gate_table, spill):
    experts_all = lax.axis_size("expert")
    own_rows, width = tokens.shape[1:]
    chips = experts_all // CORES
    scale = token_scales(
        expert_ids, gate_index, gate_table, spill, own_rows, experts_all
    )
    anywhere = pl.BlockSpec(memory_space=pl.ANY)
    vmem = pl.BlockSpec(memory_space=pltpu.VMEM)
    return pl.pallas_call(
        functools.partial(line_kernel, chips),
        out_shape=jax.ShapeDtypeStruct(tokens.shape, tokens.dtype),
        in_specs=[anywhere] * 4 + [vmem],
        out_specs=vmem,
        scratch_shapes=scratch_of(
            chips, own_rows, width, w_gate.shape[2], experts_all, tokens.dtype
        ),
        compiler_params=pltpu.CompilerParams(
            collective_id=0, has_side_effects=True, vmem_limit_bytes=67043328
        ),
    )(tokens, w_gate, w_up, w_down, scale)


def local(tokens, w_gate, w_up, w_down, *routing):
    own_rows, width = tokens.shape[1:]
    experts_all = lax.axis_size("expert")
    held = w_gate.size + w_up.size + w_down.size + 4 * experts_all * own_rows * width
    fits = held * tokens.dtype.itemsize <= 56 * 2**20
    if fits and w_gate.shape[0] == 1 and experts_all % CORES == 0:
        return line_plan(tokens, w_gate, w_up, w_down, *routing)
    return exchange_plan(tokens, w_gate, w_up, w_down, *routing)


def solution(mesh):
    in_specs = (
        P("expert", "dp", None),
        P("expert", None, None),
        P("expert", None, None),
        P("expert", None, None),
        P("expert", None, None),
        P("expert", None, None),
        P(),
        P("expert", None),
    )
    out_specs = P("expert", "dp", None)
    return jax.shard_map(local, mesh=mesh, in_specs=in_specs, out_specs=out_specs, check_vma=False)
```

```python
import functools
import jax
import jax.numpy as jnp
from jax import lax
from jax.experimental import pallas as pl
from jax.experimental.pallas import tpu as pltpu
from jax.sharding import PartitionSpec as P


def exchange_plan(tokens, w_gate, w_up, w_down, expert_ids, gate_index, gate_table, spill):
    dp_count = lax.axis_size("dp")
    expert_count = lax.axis_size("expert")
    local_experts = w_gate.shape[0]
    experts_all = local_experts * expert_count
    own_rows = tokens.shape[1]
    model_width = tokens.shape[2]
    column_tokens = spill.shape[1]
    top_count = expert_ids.shape[2]
    capacity = 3 * own_rows * top_count // (2 * experts_all)
    spill_room = own_rows // 4
    dp_index = lax.axis_index("dp")
    senders = spill[0]
    flat_ids = expert_ids[0].reshape(-1)
    level_count = gate_table.shape[0]
    matches = gate_index[0][:, :, None] == jnp.arange(level_count, dtype=jnp.int32)
    picked = jnp.sum(jnp.where(matches, gate_table, 0.0), axis=2)
    weight = picked / jnp.sum(picked, axis=1, keepdims=True)
    pair_sender = jnp.repeat(senders, top_count)
    is_mine = pair_sender == dp_index
    onehot = (
        (flat_ids[:, None] == jnp.arange(experts_all, dtype=jnp.int32)) & is_mine[:, None]
    ).astype(jnp.int32)
    slot_rank = jnp.sum((jnp.cumsum(onehot, axis=0) - onehot) * onehot, axis=1)
    is_kept = is_mine & (slot_rank < capacity)
    empty_slot = experts_all * capacity
    slot_index = jnp.where(is_kept, flat_ids * capacity + slot_rank, empty_slot)
    pair_token = jnp.arange(column_tokens * top_count, dtype=jnp.int32) // top_count
    zero_row = jnp.zeros((1, model_width), tokens.dtype)
    token_ids = jnp.arange(column_tokens, dtype=jnp.int32)
    home_dev = token_ids // own_rows
    local_token = token_ids - home_dev * own_rows
    is_moved = senders != home_dev
    route_key = home_dev * dp_count + senders
    route_hot = (route_key[:, None] == jnp.arange(dp_count * dp_count, dtype=jnp.int32)).astype(
        jnp.int32
    )
    spill_rank = jnp.sum((jnp.cumsum(route_hot, axis=0) - route_hot) * route_hot, axis=1)
    incoming = is_moved & (senders == dp_index)
    spill_slots = dp_count * spill_room
    outgoing = is_moved & (home_dev == dp_index)
    send_target = jnp.where(outgoing, senders * spill_room + spill_rank, spill_slots)
    send_source = (
        jnp.full((spill_slots,), own_rows, jnp.int32).at[send_target].set(local_token, mode="drop")
    )
    own_padded = jnp.concatenate([tokens[0], zero_row], axis=0)
    outgoing_rows = own_padded[send_source].reshape(dp_count, spill_room, model_width)
    arrived = lax.all_to_all(outgoing_rows, "dp", split_axis=0, concat_axis=0, tiled=True)
    source_rows = jnp.concatenate(
        [tokens[0], arrived.reshape(spill_slots, model_width), zero_row], axis=0
    )
    token_row = jnp.where(
        home_dev == dp_index,
        local_token,
        jnp.where(incoming, own_rows + home_dev * spill_room + spill_rank, own_rows + spill_slots),
    )
    dispatch_source = (
        jnp.full((empty_slot,), source_rows.shape[0] - 1, jnp.int32)
        .at[slot_index]
        .set(token_row[pair_token], mode="drop")
    )
    outbound = source_rows[dispatch_source].reshape(
        expert_count, local_experts, capacity, model_width
    )
    block = lax.all_to_all(outbound, "expert", split_axis=0, concat_axis=0, tiled=True)
    gate_part = jnp.einsum("aecd,edf->aecf", block, w_gate, preferred_element_type=jnp.float32)
    up_part = jnp.einsum("aecd,edf->aecf", block, w_up, preferred_element_type=jnp.float32)
    hidden = (jax.nn.silu(gate_part) * up_part).astype(jnp.bfloat16)
    expert_out = jnp.einsum(
        "aecf,efd->aecd", hidden, w_down, preferred_element_type=jnp.float32
    ).astype(jnp.bfloat16)
    returned = lax.all_to_all(expert_out, "expert", split_axis=0, concat_axis=0, tiled=True)
    results = jnp.concatenate([returned.reshape(empty_slot, model_width), zero_row], axis=0)
    slot_grid = jnp.concatenate(
        [
            slot_index.reshape(column_tokens, top_count),
            jnp.full((1, top_count), empty_slot, jnp.int32),
        ],
        axis=0,
    )
    kept_scale = jnp.where(is_kept.reshape(column_tokens, top_count), weight, 0.0)
    scale_grid = jnp.concatenate([kept_scale, jnp.zeros((1, top_count), jnp.float32)], axis=0)

    def combine(chosen):
        chosen_slots = slot_grid[chosen]
        chosen_scale = scale_grid[chosen]
        summed = jnp.zeros((chosen.shape[0], model_width), jnp.float32)
        for member in range(top_count):
            summed = summed + chosen_scale[:, member : member + 1] * results[
                chosen_slots[:, member]
            ].astype(jnp.float32)
        return summed

    own_ids = dp_index * own_rows + jnp.arange(own_rows, dtype=jnp.int32)
    own_part = combine(own_ids)
    arrived_target = jnp.where(incoming, home_dev * spill_room + spill_rank, spill_slots)
    arrived_ids = (
        jnp.full((spill_slots,), column_tokens, jnp.int32)
        .at[arrived_target]
        .set(token_ids, mode="drop")
    )
    arrived_part = combine(arrived_ids).reshape(dp_count, spill_room, model_width)
    returned_part = lax.all_to_all(
        arrived_part.astype(jnp.bfloat16), "dp", split_axis=0, concat_axis=0, tiled=True
    ).astype(arrived_part.dtype)
    back_rows = jnp.concatenate(
        [returned_part.reshape(spill_slots, model_width), jnp.zeros((1, model_width), jnp.float32)],
        axis=0,
    )
    back_pick = jnp.where(
        is_moved[own_ids], senders[own_ids] * spill_room + spill_rank[own_ids], spill_slots
    )
    mixed = own_part + back_rows[back_pick]
    return mixed.astype(jnp.bfloat16)[None]


CORES = 2
CHUNKS = 8
LAG = 2
MESH = pl.DeviceIdType.MESH


def token_scales(expert_ids, gate_index, gate_table, spill, own_rows, experts_all):
    top_count = expert_ids.shape[2]
    column_tokens = spill.shape[1]
    capacity = 3 * own_rows * top_count // (2 * experts_all)
    first = lax.axis_index("dp") * own_rows
    senders = spill[0]
    experts = jnp.arange(experts_all, dtype=jnp.int32)
    hot = expert_ids[0][:, :, None] == experts
    chosen = jnp.any(hot, axis=1)
    own_senders = lax.dynamic_slice_in_dim(senders, first, own_rows)
    own_tokens = first + jnp.arange(own_rows, dtype=jnp.int32)
    earlier = (jnp.arange(column_tokens, dtype=jnp.int32)[None, :] < own_tokens[:, None]) & (
        senders[None, :] == own_senders[:, None]
    )
    rank = jnp.dot(
        earlier.astype(jnp.bfloat16), chosen.astype(jnp.bfloat16), preferred_element_type=jnp.float32
    )
    own_index = lax.dynamic_slice_in_dim(gate_index[0], first, own_rows)
    levels = jnp.arange(gate_table.shape[0], dtype=jnp.int32)
    picked = jnp.sum(jnp.where(own_index[:, :, None] == levels, gate_table, 0.0), axis=2)
    weight = picked / jnp.sum(picked, axis=1, keepdims=True)
    own_hot = lax.dynamic_slice_in_dim(hot, first, own_rows)
    scale = jnp.sum(jnp.where(own_hot, weight[:, :, None], 0.0), axis=1)
    return jnp.where(rank < capacity, scale, 0.0).T


def line_kernel(
    chips, tok, w_gate, w_up, w_down, scale, out,
    x, w_in, w_out, scales, both, hid, part, near, from_left, from_right, going, total,
    own_sem, sc_s, sc_r, ag_right, ag_left, ag_r, ag_sib, sib_r, part_s, part_r, go_s, left_r, right_r,
):
    own_rows, width = tok.shape[1], tok.shape[2]
    hidden_units = w_gate.shape[2]
    piece = own_rows // CHUNKS
    count = chips * CORES
    me = lax.axis_index("expert")
    p = me // CORES
    q = lax.rem(me, CORES)
    sib = p * CORES + 1 - q
    right, left = me + CORES, me - CORES
    has_right, has_left = p < chips - 1, p > 0

    def send(src, dst, send_sem, recv_sem, device):
        return pltpu.make_async_remote_copy(
            src_ref=src, dst_ref=dst, send_sem=send_sem, recv_sem=recv_sem,
            device_id={"expert": device}, device_id_type=MESH,
        )

    def rows(c):
        return pl.ds(pl.multiple_of(c * piece, piece), piece)

    def gather_copy(s, c, sems, recv, device):
        block = x.at[CORES * s + q, rows(c)]
        return send(block, block, sems.at[s, c], recv.at[s, c], device)

    loads = [
        pltpu.make_async_copy(tok.at[0], x.at[me], own_sem.at[0]),
        pltpu.make_async_copy(scale, scales.at[me], own_sem.at[1]),
        pltpu.make_async_copy(w_gate.at[0], w_in.at[:, pl.ds(0, hidden_units)], own_sem.at[2]),
        pltpu.make_async_copy(w_up.at[0], w_in.at[:, pl.ds(hidden_units, hidden_units)], own_sem.at[3]),
        pltpu.make_async_copy(w_down.at[0], w_out, own_sem.at[4]),
    ]
    for load in loads:
        load.start()
    barrier = pltpu.get_barrier_semaphore()
    for step in range(1, count):
        pl.semaphore_signal(
            barrier, inc=1, device_id={"expert": lax.rem(me + step, count)}, device_id_type=MESH
        )
    pl.semaphore_wait(barrier, count - 1)
    loads[0].wait()
    for step in range(1, count):
        send(
            scale, scales.at[me], sc_s.at[step], sc_r.at[step], lax.rem(me + step, count)
        ).start()

    def first_sends(c, carry):
        @pl.when(has_right)
        def _():
            gather_copy(p, c, ag_right, ag_r, right).start()

        @pl.when(has_left)
        def _():
            gather_copy(p, c, ag_left, ag_r, left).start()

        gather_copy(p, c, ag_sib, sib_r, sib).start()
        return carry

    lax.fori_loop(0, CHUNKS, first_sends, 0)
    for load in loads[1:]:
        load.wait()
    for step in range(1, count):
        send(
            scale, scales.at[lax.rem(me - step + count, count)], sc_s.at[step], sc_r.at[step], sib
        ).wait_recv()

    tall = CORES * own_rows
    in_tile = 2 * hidden_units // 7 if (2 * hidden_units) % 7 == 0 else 2 * hidden_units
    out_tile = width // 8

    def sib_wait(s):
        def one(c, carry):
            block = x.at[CORES * s + 1 - q, rows(c)]
            send(block, block, ag_sib.at[s, c], sib_r.at[s, c], sib).wait_recv()
            return carry

        lax.fori_loop(0, CHUNKS, one, 0)

    def expert(s):
        def enter(t, carry):
            cols = pl.ds(pl.multiple_of(t * in_tile, 128), in_tile)
            tokens = x[pl.ds(CORES * s, CORES)].reshape(tall, width)
            both[:, cols] = jnp.dot(tokens, w_in[:, cols], preferred_element_type=jnp.float32)
            return carry

        lax.fori_loop(0, 2 * hidden_units // in_tile, enter, 0)
        for core in range(CORES):
            part_rows = pl.ds(core * own_rows, own_rows)
            row = scales[CORES * s + core, pl.ds(me, 1), :]
            col = jnp.transpose(jnp.broadcast_to(row, (own_rows, own_rows)))[:, :1]
            gate = both[part_rows, pl.ds(0, hidden_units)]
            up = both[part_rows, pl.ds(hidden_units, hidden_units)]
            hid[part_rows, :] = (gate / (1.0 + jnp.exp(-gate)) * up * col).astype(hid.dtype)

        def leave(t, carry):
            cols = pl.ds(pl.multiple_of(t * out_tile, 128), out_tile)
            made = jnp.dot(hid[...], w_out[:, cols], preferred_element_type=jnp.float32)
            part[pl.ds(CORES * s, CORES), :, cols] = made.astype(part.dtype).reshape(
                CORES, own_rows, out_tile
            )
            return carry

        lax.fori_loop(0, width // out_tile, leave, 0)
        near_copy(s).start()

    def near_copy(s):
        return send(part.at[CORES * s + 1 - q], near.at[s], part_s.at[s], part_r.at[s], sib)

    def pair_sum(s, c):
        return part[CORES * s + q, rows(c)].astype(jnp.float32) + near[s, rows(c)].astype(jnp.float32)

    def onward(s, c, has_up, came, came_sem, device):
        @pl.when(c == 0)
        def _():
            near_copy(s).wait_recv()

        total[...] = pair_sum(s, c)

        @pl.when(has_up)
        def _():
            send(
                going.at[s, rows(c)], came.at[s, rows(c)], go_s.at[s, c], came_sem.at[s, c], sib
            ).wait_recv()
            total[...] += came[s, rows(c)].astype(jnp.float32)

        going[s, rows(c)] = total[...].astype(going.dtype)
        send(
            going.at[s, rows(c)], came.at[s, rows(c)], go_s.at[s, c], came_sem.at[s, c], device
        ).start()

    def slot(k, carry):
        for side in range(2):
            s = p - k if side == 0 else p + k
            valid = (s >= 0) if side == 0 else ((s < chips) & (k > 0))

            @pl.when(valid)
            def _():
                sib_wait(s)
                expert(s)

        def step(i, inner):
            to_right = i - LAG * p

            @pl.when((p < k) & (to_right >= 0) & (to_right < CHUNKS))
            def _():
                onward(k, to_right, has_left, from_left, left_r, right)

            to_left = i - LAG * (chips - 1 - p)
            low = chips - 1 - k

            @pl.when((p > low) & (to_left >= 0) & (to_left < CHUNKS))
            def _():
                onward(low, to_left, has_right, from_right, right_r, left)

            before = p - k - 1

            @pl.when((i < CHUNKS) & (before >= 0))
            def _():
                gather_copy(before, i, ag_right, ag_r, sib).wait_recv()

                @pl.when(has_right)
                def _():
                    gather_copy(before, i, ag_right, ag_r, right).start()

                gather_copy(before, i, ag_sib, sib_r, sib).start()

            after = p + k + 1

            @pl.when((i < CHUNKS) & (after < chips))
            def _():
                gather_copy(after, i, ag_left, ag_r, sib).wait_recv()

                @pl.when(has_left)
                def _():
                    gather_copy(after, i, ag_left, ag_r, left).start()

                gather_copy(after, i, ag_sib, sib_r, sib).start()

            return inner

        lax.fori_loop(0, CHUNKS + LAG * (chips - 1), step, 0)
        return carry

    lax.fori_loop(0, chips, slot, 0)
    near_copy(p).wait_recv()

    def finish(c, carry):
        total[...] = pair_sum(p, c)

        @pl.when(has_left)
        def _():
            block = from_left.at[p, rows(c)]
            send(block, block, go_s.at[p, c], left_r.at[p, c], sib).wait_recv()
            total[...] += from_left[p, rows(c)].astype(jnp.float32)

        @pl.when(has_right)
        def _():
            block = from_right.at[p, rows(c)]
            send(block, block, go_s.at[p, c], right_r.at[p, c], sib).wait_recv()
            total[...] += from_right[p, rows(c)].astype(jnp.float32)

        out[0, rows(c)] = total[...].astype(out.dtype)
        return carry

    lax.fori_loop(0, CHUNKS, finish, 0)

    for step in range(1, count):
        send(scale, scales.at[me], sc_s.at[step], sc_r.at[step], sib).wait_send()

    def drain(s, carry):
        near_copy(s).wait_send()

        def one(c, inner):
            gather_copy(s, c, ag_sib, sib_r, sib).wait_send()

            @pl.when(has_right & (s <= p))
            def _():
                gather_copy(s, c, ag_right, ag_r, sib).wait_send()

            @pl.when(has_left & (s >= p))
            def _():
                gather_copy(s, c, ag_left, ag_r, sib).wait_send()

            @pl.when(s != p)
            def _():
                block = going.at[s, rows(c)]
                send(block, block, go_s.at[s, c], left_r.at[s, c], sib).wait_send()

            return inner

        lax.fori_loop(0, CHUNKS, one, 0)
        return carry

    lax.fori_loop(0, chips, drain, 0)


def scratch_of(chips, own_rows, width, hidden_units, experts_all, dtype):
    count = chips * CORES
    blocks = pltpu.VMEM((count, own_rows, width), dtype)
    halves = pltpu.VMEM((chips, own_rows, width), dtype)
    dma = pltpu.SemaphoreType.DMA
    grid = dma((chips, CHUNKS))
    return [
        blocks,
        pltpu.VMEM((width, 2 * hidden_units), dtype),
        pltpu.VMEM((hidden_units, width), dtype),
        pltpu.VMEM((count, experts_all, own_rows), jnp.float32),
        pltpu.VMEM((CORES * own_rows, 2 * hidden_units), jnp.float32),
        pltpu.VMEM((CORES * own_rows, hidden_units), dtype),
        blocks,
        halves,
        halves,
        halves,
        halves,
        pltpu.VMEM((own_rows // CHUNKS, width), jnp.float32),
        dma((5,)),
        dma((count,)),
        dma((count,)),
        grid, grid, grid, grid, grid,
        dma((chips,)),
        dma((chips,)),
        grid, grid, grid,
    ]


def line_plan(tokens, w_gate, w_up, w_down, expert_ids, gate_index, gate_table, spill):
    experts_all = lax.axis_size("expert")
    own_rows, width = tokens.shape[1:]
    chips = experts_all // CORES
    scale = token_scales(
        expert_ids, gate_index, gate_table, spill, own_rows, experts_all
    )
    anywhere = pl.BlockSpec(memory_space=pl.ANY)
    vmem = pl.BlockSpec(memory_space=pltpu.VMEM)
    return pl.pallas_call(
        functools.partial(line_kernel, chips),
        out_shape=jax.ShapeDtypeStruct(tokens.shape, tokens.dtype),
        in_specs=[anywhere] * 4 + [vmem],
        out_specs=vmem,
        scratch_shapes=scratch_of(
            chips, own_rows, width, w_gate.shape[2], experts_all, tokens.dtype
        ),
        compiler_params=pltpu.CompilerParams(
            collective_id=0, has_side_effects=True, vmem_limit_bytes=67043328
        ),
    )(tokens, w_gate, w_up, w_down, scale)


def local(tokens, w_gate, w_up, w_down, *routing):
    own_rows, width = tokens.shape[1:]
    experts_all = lax.axis_size("expert")
    held = w_gate.size + w_up.size + w_down.size + 4 * experts_all * own_rows * width
    fits = held * tokens.dtype.itemsize <= 56 * 2**20
    if fits and w_gate.shape[0] == 1 and experts_all % CORES == 0:
        return line_plan(tokens, w_gate, w_up, w_down, *routing)
    return exchange_plan(tokens, w_gate, w_up, w_down, *routing)


def solution(mesh):
    in_specs = (
        P("expert", "dp", None),
        P("expert", None, None),
        P("expert", None, None),
        P("expert", None, None),
        P("expert", None, None),
        P("expert", None, None),
        P(),
        P("expert", None),
    )
    out_specs = P("expert", "dp", None)
    return jax.shard_map(local, mesh=mesh, in_specs=in_specs, out_specs=out_specs, check_vma=False)
```

```python
import functools
import jax
import jax.numpy as jnp
from jax import lax
from jax.experimental import pallas as pl
from jax.experimental.pallas import tpu as pltpu
from jax.sharding import PartitionSpec as P


def exchange_plan(tokens, w_gate, w_up, w_down, expert_ids, gate_index, gate_table, spill):
    dp_count = lax.axis_size("dp")
    expert_count = lax.axis_size("expert")
    local_experts = w_gate.shape[0]
    experts_all = local_experts * expert_count
    own_rows = tokens.shape[1]
    model_width = tokens.shape[2]
    column_tokens = spill.shape[1]
    top_count = expert_ids.shape[2]
    capacity = 3 * own_rows * top_count // (2 * experts_all)
    spill_room = own_rows // 4
    dp_index = lax.axis_index("dp")
    senders = spill[0]
    flat_ids = expert_ids[0].reshape(-1)
    level_count = gate_table.shape[0]
    matches = gate_index[0][:, :, None] == jnp.arange(level_count, dtype=jnp.int32)
    picked = jnp.sum(jnp.where(matches, gate_table, 0.0), axis=2)
    weight = picked / jnp.sum(picked, axis=1, keepdims=True)
    pair_sender = jnp.repeat(senders, top_count)
    is_mine = pair_sender == dp_index
    onehot = (
        (flat_ids[:, None] == jnp.arange(experts_all, dtype=jnp.int32)) & is_mine[:, None]
    ).astype(jnp.int32)
    slot_rank = jnp.sum((jnp.cumsum(onehot, axis=0) - onehot) * onehot, axis=1)
    is_kept = is_mine & (slot_rank < capacity)
    empty_slot = experts_all * capacity
    slot_index = jnp.where(is_kept, flat_ids * capacity + slot_rank, empty_slot)
    pair_token = jnp.arange(column_tokens * top_count, dtype=jnp.int32) // top_count
    zero_row = jnp.zeros((1, model_width), tokens.dtype)
    token_ids = jnp.arange(column_tokens, dtype=jnp.int32)
    home_dev = token_ids // own_rows
    local_token = token_ids - home_dev * own_rows
    is_moved = senders != home_dev
    route_key = home_dev * dp_count + senders
    route_hot = (route_key[:, None] == jnp.arange(dp_count * dp_count, dtype=jnp.int32)).astype(
        jnp.int32
    )
    spill_rank = jnp.sum((jnp.cumsum(route_hot, axis=0) - route_hot) * route_hot, axis=1)
    incoming = is_moved & (senders == dp_index)
    spill_slots = dp_count * spill_room
    outgoing = is_moved & (home_dev == dp_index)
    send_target = jnp.where(outgoing, senders * spill_room + spill_rank, spill_slots)
    send_source = (
        jnp.full((spill_slots,), own_rows, jnp.int32).at[send_target].set(local_token, mode="drop")
    )
    own_padded = jnp.concatenate([tokens[0], zero_row], axis=0)
    outgoing_rows = own_padded[send_source].reshape(dp_count, spill_room, model_width)
    arrived = lax.all_to_all(outgoing_rows, "dp", split_axis=0, concat_axis=0, tiled=True)
    source_rows = jnp.concatenate(
        [tokens[0], arrived.reshape(spill_slots, model_width), zero_row], axis=0
    )
    token_row = jnp.where(
        home_dev == dp_index,
        local_token,
        jnp.where(incoming, own_rows + home_dev * spill_room + spill_rank, own_rows + spill_slots),
    )
    dispatch_source = (
        jnp.full((empty_slot,), source_rows.shape[0] - 1, jnp.int32)
        .at[slot_index]
        .set(token_row[pair_token], mode="drop")
    )
    outbound = source_rows[dispatch_source].reshape(
        expert_count, local_experts, capacity, model_width
    )
    block = lax.all_to_all(outbound, "expert", split_axis=0, concat_axis=0, tiled=True)
    gate_part = jnp.einsum("aecd,edf->aecf", block, w_gate, preferred_element_type=jnp.float32)
    up_part = jnp.einsum("aecd,edf->aecf", block, w_up, preferred_element_type=jnp.float32)
    hidden = (jax.nn.silu(gate_part) * up_part).astype(jnp.bfloat16)
    expert_out = jnp.einsum(
        "aecf,efd->aecd", hidden, w_down, preferred_element_type=jnp.float32
    ).astype(jnp.bfloat16)
    returned = lax.all_to_all(expert_out, "expert", split_axis=0, concat_axis=0, tiled=True)
    results = jnp.concatenate([returned.reshape(empty_slot, model_width), zero_row], axis=0)
    slot_grid = jnp.concatenate(
        [
            slot_index.reshape(column_tokens, top_count),
            jnp.full((1, top_count), empty_slot, jnp.int32),
        ],
        axis=0,
    )
    kept_scale = jnp.where(is_kept.reshape(column_tokens, top_count), weight, 0.0)
    scale_grid = jnp.concatenate([kept_scale, jnp.zeros((1, top_count), jnp.float32)], axis=0)

    def combine(chosen):
        chosen_slots = slot_grid[chosen]
        chosen_scale = scale_grid[chosen]
        summed = jnp.zeros((chosen.shape[0], model_width), jnp.float32)
        for member in range(top_count):
            summed = summed + chosen_scale[:, member : member + 1] * results[
                chosen_slots[:, member]
            ].astype(jnp.float32)
        return summed

    own_ids = dp_index * own_rows + jnp.arange(own_rows, dtype=jnp.int32)
    own_part = combine(own_ids)
    arrived_target = jnp.where(incoming, home_dev * spill_room + spill_rank, spill_slots)
    arrived_ids = (
        jnp.full((spill_slots,), column_tokens, jnp.int32)
        .at[arrived_target]
        .set(token_ids, mode="drop")
    )
    arrived_part = combine(arrived_ids).reshape(dp_count, spill_room, model_width)
    returned_part = lax.all_to_all(
        arrived_part.astype(jnp.bfloat16), "dp", split_axis=0, concat_axis=0, tiled=True
    ).astype(arrived_part.dtype)
    back_rows = jnp.concatenate(
        [returned_part.reshape(spill_slots, model_width), jnp.zeros((1, model_width), jnp.float32)],
        axis=0,
    )
    back_pick = jnp.where(
        is_moved[own_ids], senders[own_ids] * spill_room + spill_rank[own_ids], spill_slots
    )
    mixed = own_part + back_rows[back_pick]
    return mixed.astype(jnp.bfloat16)[None]


CORES = 2
CHUNKS = 4
TILES = 8
LEAVE = 4
LAG = 2
MESH = pl.DeviceIdType.MESH


def token_scales(expert_ids, gate_index, gate_table, spill, own_rows, experts_all):
    top_count = expert_ids.shape[2]
    column_tokens = spill.shape[1]
    capacity = 3 * own_rows * top_count // (2 * experts_all)
    first = lax.axis_index("dp") * own_rows
    senders = spill[0]
    experts = jnp.arange(experts_all, dtype=jnp.int32)
    hot = expert_ids[0][:, :, None] == experts
    chosen = jnp.any(hot, axis=1)
    own_senders = lax.dynamic_slice_in_dim(senders, first, own_rows)
    own_tokens = first + jnp.arange(own_rows, dtype=jnp.int32)
    earlier = (jnp.arange(column_tokens, dtype=jnp.int32)[None, :] < own_tokens[:, None]) & (
        senders[None, :] == own_senders[:, None]
    )
    rank = jnp.dot(
        earlier.astype(jnp.bfloat16), chosen.astype(jnp.bfloat16), preferred_element_type=jnp.float32
    )
    own_index = lax.dynamic_slice_in_dim(gate_index[0], first, own_rows)
    levels = jnp.arange(gate_table.shape[0], dtype=jnp.int32)
    picked = jnp.sum(jnp.where(own_index[:, :, None] == levels, gate_table, 0.0), axis=2)
    weight = picked / jnp.sum(picked, axis=1, keepdims=True)
    own_hot = lax.dynamic_slice_in_dim(hot, first, own_rows)
    scale = jnp.sum(jnp.where(own_hot, weight[:, :, None], 0.0), axis=1)
    return jnp.where(rank < capacity, scale, 0.0).T


def line_kernel(
    chips, tok, w_gate, w_up, w_down, scale, out,
    x, w_in, w_out, scales, both, hid, part, near, from_left, from_right, going, total,
    own_sem, sc_s, sc_r, ag_right, ag_left, ag_r, ag_sib, sib_r, part_s, part_r, go_s, left_r, right_r,
):
    own_rows, width = tok.shape[1], tok.shape[2]
    hidden_units = w_gate.shape[2]
    piece = own_rows // CHUNKS
    tile = width // TILES
    count = chips * CORES
    me = lax.axis_index("expert")
    p = me // CORES
    q = lax.rem(me, CORES)
    sib = p * CORES + 1 - q
    right, left = me + CORES, me - CORES
    has_right, has_left = p < chips - 1, p > 0

    def send(src, dst, send_sem, recv_sem, device):
        return pltpu.make_async_remote_copy(
            src_ref=src, dst_ref=dst, send_sem=send_sem, recv_sem=recv_sem,
            device_id={"expert": device}, device_id_type=MESH,
        )

    def rows(c):
        return pl.ds(pl.multiple_of(c * piece, piece), piece)

    def gather_copy(s, c, sems, recv, device):
        block = x.at[CORES * s + q, rows(c)]
        return send(block, block, sems.at[s, c], recv.at[s, c], device)

    loads = [
        pltpu.make_async_copy(tok.at[0], x.at[me], own_sem.at[0]),
        pltpu.make_async_copy(scale, scales.at[me], own_sem.at[1]),
        pltpu.make_async_copy(w_gate.at[0], w_in.at[:, pl.ds(0, hidden_units)], own_sem.at[2]),
        pltpu.make_async_copy(w_up.at[0], w_in.at[:, pl.ds(hidden_units, hidden_units)], own_sem.at[3]),
        pltpu.make_async_copy(w_down.at[0], w_out, own_sem.at[4]),
    ]
    for load in loads:
        load.start()
    barrier = pltpu.get_barrier_semaphore()
    for step in range(1, count):
        pl.semaphore_signal(
            barrier, inc=1, device_id={"expert": lax.rem(me + step, count)}, device_id_type=MESH
        )
    pl.semaphore_wait(barrier, count - 1)
    loads[0].wait()
    for step in range(1, count):
        send(
            scale, scales.at[me], sc_s.at[step], sc_r.at[step], lax.rem(me + step, count)
        ).start()

    def first_sends(c, carry):
        @pl.when(has_right)
        def _():
            gather_copy(p, c, ag_right, ag_r, right).start()

        @pl.when(has_left)
        def _():
            gather_copy(p, c, ag_left, ag_r, left).start()

        gather_copy(p, c, ag_sib, sib_r, sib).start()
        return carry

    lax.fori_loop(0, CHUNKS, first_sends, 0)
    for load in loads[1:]:
        load.wait()
    for step in range(1, count):
        send(
            scale, scales.at[lax.rem(me - step + count, count)], sc_s.at[step], sc_r.at[step], sib
        ).wait_recv()

    tall = CORES * own_rows
    in_tile = hidden_units
    out_tile = width // LEAVE
    per_leave = TILES // LEAVE

    def sib_wait(s):
        def one(c, carry):
            block = x.at[CORES * s + 1 - q, rows(c)]
            send(block, block, ag_sib.at[s, c], sib_r.at[s, c], sib).wait_recv()
            return carry

        lax.fori_loop(0, CHUNKS, one, 0)

    def expert(s):
        def enter(t, carry):
            cols = pl.ds(pl.multiple_of(t * in_tile, 128), in_tile)
            tokens = x[pl.ds(CORES * s, CORES)].reshape(tall, width)
            both[:, cols] = jnp.dot(tokens, w_in[:, cols], preferred_element_type=jnp.float32)
            return carry

        lax.fori_loop(0, 2 * hidden_units // in_tile, enter, 0)
        for core in range(CORES):
            part_rows = pl.ds(core * own_rows, own_rows)
            row = scales[CORES * s + core, pl.ds(me, 1), :]
            col = jnp.transpose(jnp.broadcast_to(row, (own_rows, own_rows)))[:, :1]
            gate = both[part_rows, pl.ds(0, hidden_units)]
            up = both[part_rows, pl.ds(hidden_units, hidden_units)]
            hid[part_rows, :] = (gate / (1.0 + jnp.exp(-gate)) * up * col).astype(hid.dtype)

        def pass_on(first):
            for c in range(per_leave):
                @pl.when((p == 0) & (s > p))
                def _():
                    onward(s, first + c, None, from_left, left_r, right)

                @pl.when((p == chips - 1) & (s < p))
                def _():
                    onward(s, first + c, None, from_right, right_r, left)

        def leave(t, carry):
            cols = pl.ds(pl.multiple_of(t * out_tile, 128), out_tile)
            made = jnp.dot(hid[...], w_out[:, cols], preferred_element_type=jnp.float32)
            made = made.astype(part.dtype).reshape(CORES, own_rows, out_tile)
            for c in range(per_leave):
                at = t * per_leave + c
                part[pl.ds(CORES * s, CORES), at] = made[:, :, c * tile : (c + 1) * tile]
                near_copy(s, at).start()

            @pl.when(t > 0)
            def _():
                pass_on((t - 1) * per_leave)

            return carry

        lax.fori_loop(0, LEAVE, leave, 0)
        pass_on(TILES - per_leave)

    def near_copy(s, c):
        return send(
            part.at[CORES * s + 1 - q, c], near.at[s, c], part_s.at[s, c], part_r.at[s, c], sib
        )

    def pair_sum(s, c):
        near_copy(s, c).wait_recv()
        return part[CORES * s + q, c].astype(jnp.float32) + near[s, c].astype(jnp.float32)

    def onward(s, c, up_sem, came, came_sem, device):
        if up_sem is None:
            going[s, c] = pair_sum(s, c).astype(going.dtype)
        else:
            block = going.at[s, c]
            send(block, came.at[s, c], go_s.at[s, c], up_sem.at[s, c], sib).wait_recv()
            going[s, c] = (pair_sum(s, c) + came[s, c].astype(jnp.float32)).astype(going.dtype)
        send(
            going.at[s, c], came.at[s, c], go_s.at[s, c], came_sem.at[s, c], device
        ).start()

    def slot(k, carry):
        for side in range(2):
            s = p - k if side == 0 else p + k
            valid = (s >= 0) if side == 0 else ((s < chips) & (k > 0))

            @pl.when(valid)
            def _():
                sib_wait(s)
                expert(s)

        def step(i, inner):
            to_right = i - LAG * (p - 1)

            @pl.when((p > 0) & (p < k) & (to_right >= 0) & (to_right < TILES))
            def _():
                onward(k, to_right, left_r, from_left, left_r, right)

            to_left = i - LAG * (chips - 2 - p)
            low = chips - 1 - k

            @pl.when((p < chips - 1) & (p > low) & (to_left >= 0) & (to_left < TILES))
            def _():
                onward(low, to_left, right_r, from_right, right_r, left)

            turn = TILES // CHUNKS
            gather = lax.rem(i, turn) == turn - 1
            g = i // turn

            before = p - k - 1

            @pl.when(gather & (g < CHUNKS) & (before >= 0))
            def _():
                gather_copy(before, g, ag_right, ag_r, sib).wait_recv()

                @pl.when(has_right)
                def _():
                    gather_copy(before, g, ag_right, ag_r, right).start()

                gather_copy(before, g, ag_sib, sib_r, sib).start()

            after = p + k + 1

            @pl.when(gather & (g < CHUNKS) & (after < chips))
            def _():
                gather_copy(after, g, ag_left, ag_r, sib).wait_recv()

                @pl.when(has_left)
                def _():
                    gather_copy(after, g, ag_left, ag_r, left).start()

                gather_copy(after, g, ag_sib, sib_r, sib).start()

            return inner

        lax.fori_loop(0, TILES + LAG * max(chips - 2, 0), step, 0)
        return carry

    lax.fori_loop(0, chips, slot, 0)

    def finish(c, carry):
        total[...] = pair_sum(p, c)
        for there, came, came_sem in (
            (has_left, from_left, left_r), (has_right, from_right, right_r)
        ):
            @pl.when(there)
            def _():
                block = came.at[p, c]
                send(block, block, go_s.at[p, c], came_sem.at[p, c], sib).wait_recv()
                total[...] += came[p, c].astype(jnp.float32)

        cols = pl.ds(pl.multiple_of(c * tile, 128), tile)
        out[0, :, cols] = total[...].astype(out.dtype)
        return carry

    lax.fori_loop(0, TILES, finish, 0)

    for step in range(1, count):
        send(scale, scales.at[me], sc_s.at[step], sc_r.at[step], sib).wait_send()

    def drain(s, carry):
        def gathered(c, inner):
            gather_copy(s, c, ag_sib, sib_r, sib).wait_send()

            @pl.when(has_right & (s <= p))
            def _():
                gather_copy(s, c, ag_right, ag_r, sib).wait_send()

            @pl.when(has_left & (s >= p))
            def _():
                gather_copy(s, c, ag_left, ag_r, sib).wait_send()

            return inner

        def summed(c, inner):
            near_copy(s, c).wait_send()

            @pl.when(s != p)
            def _():
                block = going.at[s, c]
                send(block, block, go_s.at[s, c], left_r.at[s, c], sib).wait_send()

            return inner

        lax.fori_loop(0, CHUNKS, gathered, 0)
        lax.fori_loop(0, TILES, summed, 0)
        return carry

    lax.fori_loop(0, chips, drain, 0)


def scratch_of(chips, own_rows, width, hidden_units, experts_all, dtype):
    count = chips * CORES
    tile = width // TILES
    halves = pltpu.VMEM((chips, TILES, own_rows, tile), dtype)
    dma = pltpu.SemaphoreType.DMA
    gather = dma((chips, CHUNKS))
    tiled = dma((chips, TILES))
    return [
        pltpu.VMEM((count, own_rows, width), dtype),
        pltpu.VMEM((width, 2 * hidden_units), dtype),
        pltpu.VMEM((hidden_units, width), dtype),
        pltpu.VMEM((count, experts_all, own_rows), jnp.float32),
        pltpu.VMEM((CORES * own_rows, 2 * hidden_units), jnp.float32),
        pltpu.VMEM((CORES * own_rows, hidden_units), dtype),
        pltpu.VMEM((count, TILES, own_rows, tile), dtype),
        halves,
        halves,
        halves,
        halves,
        pltpu.VMEM((own_rows, tile), jnp.float32),
        dma((5,)),
        dma((count,)),
        dma((count,)),
        gather, gather, gather, gather, gather,
        tiled, tiled, tiled, tiled, tiled,
    ]


def line_plan(tokens, w_gate, w_up, w_down, expert_ids, gate_index, gate_table, spill):
    experts_all = lax.axis_size("expert")
    own_rows, width = tokens.shape[1:]
    chips = experts_all // CORES
    scale = token_scales(
        expert_ids, gate_index, gate_table, spill, own_rows, experts_all
    )
    anywhere = pl.BlockSpec(memory_space=pl.ANY)
    vmem = pl.BlockSpec(memory_space=pltpu.VMEM)
    return pl.pallas_call(
        functools.partial(line_kernel, chips),
        out_shape=jax.ShapeDtypeStruct(tokens.shape, tokens.dtype),
        in_specs=[anywhere] * 4 + [vmem],
        out_specs=vmem,
        scratch_shapes=scratch_of(
            chips, own_rows, width, w_gate.shape[2], experts_all, tokens.dtype
        ),
        compiler_params=pltpu.CompilerParams(
            collective_id=0, has_side_effects=True, vmem_limit_bytes=67043328
        ),
    )(tokens, w_gate, w_up, w_down, scale)


def local(tokens, w_gate, w_up, w_down, *routing):
    own_rows, width = tokens.shape[1:]
    experts_all = lax.axis_size("expert")
    held = w_gate.size + w_up.size + w_down.size + 4 * experts_all * own_rows * width
    fits = held * tokens.dtype.itemsize <= 56 * 2**20
    if fits and w_gate.shape[0] == 1 and experts_all % CORES == 0:
        return line_plan(tokens, w_gate, w_up, w_down, *routing)
    return exchange_plan(tokens, w_gate, w_up, w_down, *routing)


def solution(mesh):
    in_specs = (
        P("expert", "dp", None),
        P("expert", None, None),
        P("expert", None, None),
        P("expert", None, None),
        P("expert", None, None),
        P("expert", None, None),
        P(),
        P("expert", None),
    )
    out_specs = P("expert", "dp", None)
    return jax.shard_map(local, mesh=mesh, in_specs=in_specs, out_specs=out_specs, check_vma=False)
```

```python
import functools
import jax
import jax.numpy as jnp
from jax import lax
from jax.experimental import pallas as pl
from jax.experimental.pallas import tpu as pltpu
from jax.sharding import PartitionSpec as P


def exchange_plan(tokens, w_gate, w_up, w_down, expert_ids, gate_index, gate_table, spill):
    dp_count = lax.axis_size("dp")
    expert_count = lax.axis_size("expert")
    local_experts = w_gate.shape[0]
    experts_all = local_experts * expert_count
    own_rows = tokens.shape[1]
    model_width = tokens.shape[2]
    column_tokens = spill.shape[1]
    top_count = expert_ids.shape[2]
    capacity = 3 * own_rows * top_count // (2 * experts_all)
    spill_room = own_rows // 4
    dp_index = lax.axis_index("dp")
    senders = spill[0]
    flat_ids = expert_ids[0].reshape(-1)
    level_count = gate_table.shape[0]
    matches = gate_index[0][:, :, None] == jnp.arange(level_count, dtype=jnp.int32)
    picked = jnp.sum(jnp.where(matches, gate_table, 0.0), axis=2)
    weight = picked / jnp.sum(picked, axis=1, keepdims=True)
    pair_sender = jnp.repeat(senders, top_count)
    is_mine = pair_sender == dp_index
    onehot = (
        (flat_ids[:, None] == jnp.arange(experts_all, dtype=jnp.int32)) & is_mine[:, None]
    ).astype(jnp.int32)
    slot_rank = jnp.sum((jnp.cumsum(onehot, axis=0) - onehot) * onehot, axis=1)
    is_kept = is_mine & (slot_rank < capacity)
    empty_slot = experts_all * capacity
    slot_index = jnp.where(is_kept, flat_ids * capacity + slot_rank, empty_slot)
    pair_token = jnp.arange(column_tokens * top_count, dtype=jnp.int32) // top_count
    zero_row = jnp.zeros((1, model_width), tokens.dtype)
    token_ids = jnp.arange(column_tokens, dtype=jnp.int32)
    home_dev = token_ids // own_rows
    local_token = token_ids - home_dev * own_rows
    is_moved = senders != home_dev
    route_key = home_dev * dp_count + senders
    route_hot = (route_key[:, None] == jnp.arange(dp_count * dp_count, dtype=jnp.int32)).astype(
        jnp.int32
    )
    spill_rank = jnp.sum((jnp.cumsum(route_hot, axis=0) - route_hot) * route_hot, axis=1)
    incoming = is_moved & (senders == dp_index)
    spill_slots = dp_count * spill_room
    outgoing = is_moved & (home_dev == dp_index)
    send_target = jnp.where(outgoing, senders * spill_room + spill_rank, spill_slots)
    send_source = (
        jnp.full((spill_slots,), own_rows, jnp.int32).at[send_target].set(local_token, mode="drop")
    )
    own_padded = jnp.concatenate([tokens[0], zero_row], axis=0)
    outgoing_rows = own_padded[send_source].reshape(dp_count, spill_room, model_width)
    arrived = lax.all_to_all(outgoing_rows, "dp", split_axis=0, concat_axis=0, tiled=True)
    source_rows = jnp.concatenate(
        [tokens[0], arrived.reshape(spill_slots, model_width), zero_row], axis=0
    )
    token_row = jnp.where(
        home_dev == dp_index,
        local_token,
        jnp.where(incoming, own_rows + home_dev * spill_room + spill_rank, own_rows + spill_slots),
    )
    dispatch_source = (
        jnp.full((empty_slot,), source_rows.shape[0] - 1, jnp.int32)
        .at[slot_index]
        .set(token_row[pair_token], mode="drop")
    )
    outbound = source_rows[dispatch_source].reshape(
        expert_count, local_experts, capacity, model_width
    )
    block = lax.all_to_all(outbound, "expert", split_axis=0, concat_axis=0, tiled=True)
    gate_part = jnp.einsum("aecd,edf->aecf", block, w_gate, preferred_element_type=jnp.float32)
    up_part = jnp.einsum("aecd,edf->aecf", block, w_up, preferred_element_type=jnp.float32)
    hidden = (jax.nn.silu(gate_part) * up_part).astype(jnp.bfloat16)
    expert_out = jnp.einsum(
        "aecf,efd->aecd", hidden, w_down, preferred_element_type=jnp.float32
    ).astype(jnp.bfloat16)
    returned = lax.all_to_all(expert_out, "expert", split_axis=0, concat_axis=0, tiled=True)
    results = jnp.concatenate([returned.reshape(empty_slot, model_width), zero_row], axis=0)
    slot_grid = jnp.concatenate(
        [
            slot_index.reshape(column_tokens, top_count),
            jnp.full((1, top_count), empty_slot, jnp.int32),
        ],
        axis=0,
    )
    kept_scale = jnp.where(is_kept.reshape(column_tokens, top_count), weight, 0.0)
    scale_grid = jnp.concatenate([kept_scale, jnp.zeros((1, top_count), jnp.float32)], axis=0)

    def combine(chosen):
        chosen_slots = slot_grid[chosen]
        chosen_scale = scale_grid[chosen]
        summed = jnp.zeros((chosen.shape[0], model_width), jnp.float32)
        for member in range(top_count):
            summed = summed + chosen_scale[:, member : member + 1] * results[
                chosen_slots[:, member]
            ].astype(jnp.float32)
        return summed

    own_ids = dp_index * own_rows + jnp.arange(own_rows, dtype=jnp.int32)
    own_part = combine(own_ids)
    arrived_target = jnp.where(incoming, home_dev * spill_room + spill_rank, spill_slots)
    arrived_ids = (
        jnp.full((spill_slots,), column_tokens, jnp.int32)
        .at[arrived_target]
        .set(token_ids, mode="drop")
    )
    arrived_part = combine(arrived_ids).reshape(dp_count, spill_room, model_width)
    returned_part = lax.all_to_all(
        arrived_part.astype(jnp.bfloat16), "dp", split_axis=0, concat_axis=0, tiled=True
    ).astype(arrived_part.dtype)
    back_rows = jnp.concatenate(
        [returned_part.reshape(spill_slots, model_width), jnp.zeros((1, model_width), jnp.float32)],
        axis=0,
    )
    back_pick = jnp.where(
        is_moved[own_ids], senders[own_ids] * spill_room + spill_rank[own_ids], spill_slots
    )
    mixed = own_part + back_rows[back_pick]
    return mixed.astype(jnp.bfloat16)[None]


CORES = 2
CHUNKS = 4
TILES = 8
LEAVE = 4
LAG = 2
MESH = pl.DeviceIdType.MESH


def token_scales(expert_ids, gate_index, gate_table, spill, own_rows, experts_all):
    top_count, column_tokens = expert_ids.shape[1:]
    capacity = 3 * own_rows * top_count // (2 * experts_all)
    first = pl.multiple_of(lax.axis_index("dp") * own_rows, own_rows)
    own = pl.ds(first, own_rows)
    experts = lax.broadcasted_iota(jnp.int32, (experts_all, column_tokens), 0)
    chosen = jnp.zeros((experts_all, column_tokens), jnp.float32)
    for k in range(top_count):
        chosen += jnp.where(expert_ids[0, k : k + 1, :] == experts, 1.0, 0.0)
    own_row = spill[:, own].astype(jnp.float32)
    own_senders = jnp.transpose(jnp.broadcast_to(own_row, (own_rows, own_rows)))[:, :1]
    shape = (own_rows, column_tokens)
    before = lax.broadcasted_iota(jnp.int32, shape, 1) < first + lax.broadcasted_iota(
        jnp.int32, shape, 0
    )
    earlier = before & (spill[...].astype(jnp.float32) == own_senders)
    rank = lax.dot_general(
        chosen.astype(jnp.bfloat16),
        jnp.where(earlier, 1.0, 0.0).astype(jnp.bfloat16),
        (((1,), (1,)), ((), ())),
        preferred_element_type=jnp.float32,
    )
    level_count = gate_table.shape[1]
    levels = lax.broadcasted_iota(jnp.int32, (level_count, own_rows), 0)
    table = jnp.transpose(jnp.broadcast_to(gate_table[...], (own_rows, level_count)))
    picked = [
        jnp.sum(
            jnp.where(gate_index[0, k : k + 1, own] == levels, table, 0.0), axis=0, keepdims=True
        )
        for k in range(top_count)
    ]
    norm = functools.reduce(jnp.add, picked)
    own_experts = lax.broadcasted_iota(jnp.int32, (experts_all, own_rows), 0)
    scale = jnp.zeros((experts_all, own_rows), jnp.float32)
    for k in range(top_count):
        scale += jnp.where(expert_ids[0, k : k + 1, own] == own_experts, picked[k] / norm, 0.0)
    return jnp.where(rank < capacity, scale, 0.0)


def line_kernel(
    chips, tok, w_gate, w_up, w_down, expert_ids, gate_index, gate_table, spill, out,
    x, w_in, w_out, scales, both, hid, part, near, from_left, from_right, going, total,
    own_sem, sc_s, sc_r, ag_right, ag_left, ag_r, ag_sib, sib_r, part_s, part_r, go_s, left_r, right_r,
):
    own_rows, width = tok.shape[1], tok.shape[2]
    hidden_units = w_gate.shape[2]
    piece = own_rows // CHUNKS
    tile = width // TILES
    count = chips * CORES
    me = lax.axis_index("expert")
    p = me // CORES
    q = lax.rem(me, CORES)
    sib = p * CORES + 1 - q
    right, left = me + CORES, me - CORES
    has_right, has_left = p < chips - 1, p > 0

    def send(src, dst, send_sem, recv_sem, device):
        return pltpu.make_async_remote_copy(
            src_ref=src, dst_ref=dst, send_sem=send_sem, recv_sem=recv_sem,
            device_id={"expert": device}, device_id_type=MESH,
        )

    def rows(c):
        return pl.ds(pl.multiple_of(c * piece, piece), piece)

    def gather_copy(s, c, sems, recv, device):
        block = x.at[CORES * s + q, rows(c)]
        return send(block, block, sems.at[s, c], recv.at[s, c], device)

    loads = [
        pltpu.make_async_copy(tok.at[0], x.at[me], own_sem.at[0]),
        pltpu.make_async_copy(w_gate.at[0], w_in.at[:, pl.ds(0, hidden_units)], own_sem.at[1]),
        pltpu.make_async_copy(w_up.at[0], w_in.at[:, pl.ds(hidden_units, hidden_units)], own_sem.at[2]),
        pltpu.make_async_copy(w_down.at[0], w_out, own_sem.at[3]),
    ]
    for load in loads:
        load.start()
    barrier = pltpu.get_barrier_semaphore()
    for step in range(1, count):
        pl.semaphore_signal(
            barrier, inc=1, device_id={"expert": lax.rem(me + step, count)}, device_id_type=MESH
        )
    pl.semaphore_wait(barrier, count - 1)
    loads[0].wait()

    def first_sends(c, carry):
        @pl.when(has_right)
        def _():
            gather_copy(p, c, ag_right, ag_r, right).start()

        @pl.when(has_left)
        def _():
            gather_copy(p, c, ag_left, ag_r, left).start()

        gather_copy(p, c, ag_sib, sib_r, sib).start()
        return carry

    lax.fori_loop(0, 1, first_sends, 0)
    scales[me] = token_scales(expert_ids, gate_index, gate_table, spill, tok.shape[1], count)
    mine = scales.at[me]
    for step in range(1, count):
        send(mine, mine, sc_s.at[step], sc_r.at[step], lax.rem(me + step, count)).start()
    lax.fori_loop(1, CHUNKS, first_sends, 0)
    for load in loads[1:]:
        load.wait()
    for step in range(1, count):
        send(
            mine, scales.at[lax.rem(me - step + count, count)], sc_s.at[step], sc_r.at[step], sib
        ).wait_recv()

    tall = CORES * own_rows
    in_tile = hidden_units
    out_tile = width // LEAVE
    per_leave = TILES // LEAVE

    def sib_wait(s):
        def one(c, carry):
            block = x.at[CORES * s + 1 - q, rows(c)]
            send(block, block, ag_sib.at[s, c], sib_r.at[s, c], sib).wait_recv()
            return carry

        lax.fori_loop(0, CHUNKS, one, 0)

    def expert(s):
        def enter(t, carry):
            cols = pl.ds(pl.multiple_of(t * in_tile, 128), in_tile)
            tokens = x[pl.ds(CORES * s, CORES)].reshape(tall, width)
            both[:, cols] = jnp.dot(tokens, w_in[:, cols], preferred_element_type=jnp.float32)
            return carry

        lax.fori_loop(0, 2 * hidden_units // in_tile, enter, 0)
        for core in range(CORES):
            part_rows = pl.ds(core * own_rows, own_rows)
            row = scales[CORES * s + core, pl.ds(me, 1), :]
            col = jnp.transpose(jnp.broadcast_to(row, (own_rows, own_rows)))[:, :1]
            gate = both[part_rows, pl.ds(0, hidden_units)]
            up = both[part_rows, pl.ds(hidden_units, hidden_units)]
            hid[part_rows, :] = (gate / (1.0 + jnp.exp(-gate)) * up * col).astype(hid.dtype)

        def pass_on(first):
            for c in range(per_leave):
                @pl.when((p == 0) & (s > p))
                def _():
                    onward(s, first + c, None, from_left, left_r, right)

                @pl.when((p == chips - 1) & (s < p))
                def _():
                    onward(s, first + c, None, from_right, right_r, left)

        def leave(t, carry):
            cols = pl.ds(pl.multiple_of(t * out_tile, 128), out_tile)
            made = jnp.dot(hid[...], w_out[:, cols], preferred_element_type=jnp.float32)
            made = made.astype(part.dtype).reshape(CORES, own_rows, out_tile)
            for c in range(per_leave):
                at = t * per_leave + c
                part[pl.ds(CORES * s, CORES), at] = made[:, :, c * tile : (c + 1) * tile]
                near_copy(s, at).start()

            @pl.when(t > 0)
            def _():
                pass_on((t - 1) * per_leave)

            return carry

        lax.fori_loop(0, LEAVE, leave, 0)
        pass_on(TILES - per_leave)

    def near_copy(s, c):
        return send(
            part.at[CORES * s + 1 - q, c], near.at[s, c], part_s.at[s, c], part_r.at[s, c], sib
        )

    def pair_sum(s, c):
        near_copy(s, c).wait_recv()
        return part[CORES * s + q, c].astype(jnp.float32) + near[s, c].astype(jnp.float32)

    def onward(s, c, up_sem, came, came_sem, device):
        if up_sem is None:
            going[s, c] = pair_sum(s, c).astype(going.dtype)
        else:
            block = going.at[s, c]
            send(block, came.at[s, c], go_s.at[s, c], up_sem.at[s, c], sib).wait_recv()
            going[s, c] = (pair_sum(s, c) + came[s, c].astype(jnp.float32)).astype(going.dtype)
        send(
            going.at[s, c], came.at[s, c], go_s.at[s, c], came_sem.at[s, c], device
        ).start()

    def slot(k, carry):
        for side in range(2):
            s = p - k if side == 0 else p + k
            valid = (s >= 0) if side == 0 else ((s < chips) & (k > 0))

            @pl.when(valid)
            def _():
                sib_wait(s)
                expert(s)

        def step(i, inner):
            to_right = i - LAG * (p - 1)

            @pl.when((p > 0) & (p < k) & (to_right >= 0) & (to_right < TILES))
            def _():
                onward(k, to_right, left_r, from_left, left_r, right)

            to_left = i - LAG * (chips - 2 - p)
            low = chips - 1 - k

            @pl.when((p < chips - 1) & (p > low) & (to_left >= 0) & (to_left < TILES))
            def _():
                onward(low, to_left, right_r, from_right, right_r, left)

            turn = TILES // CHUNKS
            gather = lax.rem(i, turn) == turn - 1
            g = i // turn

            before = p - k - 1

            @pl.when(gather & (g < CHUNKS) & (before >= 0))
            def _():
                gather_copy(before, g, ag_right, ag_r, sib).wait_recv()

                @pl.when(has_right)
                def _():
                    gather_copy(before, g, ag_right, ag_r, right).start()

                gather_copy(before, g, ag_sib, sib_r, sib).start()

            after = p + k + 1

            @pl.when(gather & (g < CHUNKS) & (after < chips))
            def _():
                gather_copy(after, g, ag_left, ag_r, sib).wait_recv()

                @pl.when(has_left)
                def _():
                    gather_copy(after, g, ag_left, ag_r, left).start()

                gather_copy(after, g, ag_sib, sib_r, sib).start()

            return inner

        lax.fori_loop(0, TILES + LAG * max(chips - 2, 0), step, 0)
        return carry

    lax.fori_loop(0, chips, slot, 0)

    def finish(c, carry):
        total[...] = pair_sum(p, c)
        for there, came, came_sem in (
            (has_left, from_left, left_r), (has_right, from_right, right_r)
        ):
            @pl.when(there)
            def _():
                block = came.at[p, c]
                send(block, block, go_s.at[p, c], came_sem.at[p, c], sib).wait_recv()
                total[...] += came[p, c].astype(jnp.float32)

        cols = pl.ds(pl.multiple_of(c * tile, 128), tile)
        out[0, :, cols] = total[...].astype(out.dtype)
        return carry

    lax.fori_loop(0, TILES, finish, 0)

    for step in range(1, count):
        send(mine, mine, sc_s.at[step], sc_r.at[step], sib).wait_send()

    def drain(s, carry):
        def gathered(c, inner):
            gather_copy(s, c, ag_sib, sib_r, sib).wait_send()

            @pl.when(has_right & (s <= p))
            def _():
                gather_copy(s, c, ag_right, ag_r, sib).wait_send()

            @pl.when(has_left & (s >= p))
            def _():
                gather_copy(s, c, ag_left, ag_r, sib).wait_send()

            return inner

        def summed(c, inner):
            near_copy(s, c).wait_send()

            @pl.when(s != p)
            def _():
                block = going.at[s, c]
                send(block, block, go_s.at[s, c], left_r.at[s, c], sib).wait_send()

            return inner

        lax.fori_loop(0, CHUNKS, gathered, 0)
        lax.fori_loop(0, TILES, summed, 0)
        return carry

    lax.fori_loop(0, chips, drain, 0)


def scratch_of(chips, own_rows, width, hidden_units, experts_all, dtype):
    count = chips * CORES
    tile = width // TILES
    halves = pltpu.VMEM((chips, TILES, own_rows, tile), dtype)
    dma = pltpu.SemaphoreType.DMA
    gather = dma((chips, CHUNKS))
    tiled = dma((chips, TILES))
    return [
        pltpu.VMEM((count, own_rows, width), dtype),
        pltpu.VMEM((width, 2 * hidden_units), dtype),
        pltpu.VMEM((hidden_units, width), dtype),
        pltpu.VMEM((count, experts_all, own_rows), jnp.float32),
        pltpu.VMEM((CORES * own_rows, 2 * hidden_units), jnp.float32),
        pltpu.VMEM((CORES * own_rows, hidden_units), dtype),
        pltpu.VMEM((count, TILES, own_rows, tile), dtype),
        halves,
        halves,
        halves,
        halves,
        pltpu.VMEM((own_rows, tile), jnp.float32),
        dma((4,)),
        dma((count,)),
        dma((count,)),
        gather, gather, gather, gather, gather,
        tiled, tiled, tiled, tiled, tiled,
    ]


def line_plan(tokens, w_gate, w_up, w_down, expert_ids, gate_index, gate_table, spill):
    experts_all = lax.axis_size("expert")
    own_rows, width = tokens.shape[1:]
    chips = experts_all // CORES
    anywhere = pl.BlockSpec(memory_space=pl.ANY)
    vmem = pl.BlockSpec(memory_space=pltpu.VMEM)
    return pl.pallas_call(
        functools.partial(line_kernel, chips),
        out_shape=jax.ShapeDtypeStruct(tokens.shape, tokens.dtype),
        in_specs=[anywhere] * 4 + [vmem] * 4,
        out_specs=vmem,
        scratch_shapes=scratch_of(
            chips, own_rows, width, w_gate.shape[2], experts_all, tokens.dtype
        ),
        compiler_params=pltpu.CompilerParams(
            collective_id=0, has_side_effects=True, vmem_limit_bytes=67043328
        ),
    )(
        tokens, w_gate, w_up, w_down,
        jnp.swapaxes(expert_ids, 1, 2), jnp.swapaxes(gate_index, 1, 2), gate_table[None], spill,
    )


def local(tokens, w_gate, w_up, w_down, *routing):
    own_rows, width = tokens.shape[1:]
    experts_all = lax.axis_size("expert")
    held = w_gate.size + w_up.size + w_down.size + 4 * experts_all * own_rows * width
    fits = held * tokens.dtype.itemsize <= 56 * 2**20
    if fits and w_gate.shape[0] == 1 and experts_all % CORES == 0:
        return line_plan(tokens, w_gate, w_up, w_down, *routing)
    return exchange_plan(tokens, w_gate, w_up, w_down, *routing)


def solution(mesh):
    in_specs = (
        P("expert", "dp", None),
        P("expert", None, None),
        P("expert", None, None),
        P("expert", None, None),
        P("expert", None, None),
        P("expert", None, None),
        P(),
        P("expert", None),
    )
    out_specs = P("expert", "dp", None)
    return jax.shard_map(local, mesh=mesh, in_specs=in_specs, out_specs=out_specs, check_vma=False)
```
